32 devices in a mesh: section: 2 (over x), slab: 16 (over z, y, core).
Axes of the slice: x: 2, y: 2, z: 4, core: 2. Of those that a mesh axis runs over, the one named last changes fastest.
Arguments:
- concentration: float32 [4, 2048, 2048], P('section', 'slab'), may hold values from -3.2 to 3.2
Outputs:
- new_concentration: float32 [4, 2048, 2048], P('section', 'slab')
- energy: float32 [], replicated
The draws below stay inside these ranges and needn't reach their ends.
All inputs are finite; a program needn't handle non-finite values.
Results may differ from the reference program's by a relative error of at most 0.000098.
Values sent between devices are 32-bit elements; how exact they have to be, the bound alone decides.
A program may use at most 64 MiB of HBM per device.

```python
import math
import jax
import jax.numpy as jnp
from jax import lax

NX = 2048
NY = 2048
NZ = 4


def blur_weights(extent, coarse_total, blur_width):
    position = jnp.arange(extent, dtype=jnp.float32)
    spacing = extent / coarse_total
    centers = (jnp.arange(coarse_total, dtype=jnp.float32) + 0.5) * spacing
    offset = position[:, None] - centers[None, :]
    offset = jnp.mod(offset + 0.5 * extent, extent) - 0.5 * extent
    weights = jnp.exp(-offset * offset / (2.0 * blur_width * blur_width))
    return weights / jnp.sqrt(jnp.sum(weights * weights, axis=1, keepdims=True))


def draw_concentration(key, part):
    base_key = jax.random.fold_in(key, 7)
    noise_key = jax.random.fold_in(base_key, 0)
    smooth_key = jax.random.fold_in(base_key, 2)
    coarse_x = max(NX // 16, 4)
    coarse_y = max(NY // 16, 4)
    coarse = jax.random.normal(smooth_key, (NZ, coarse_x, coarse_y), jnp.float32)
    along_x = blur_weights(NX, coarse_x, 16.0)
    along_y = blur_weights(NY, coarse_y, 16.0)
    smooth = jnp.einsum('zij,xi->zxj', coarse, along_x, precision=lax.Precision.HIGHEST)
    smooth = jnp.einsum('zxj,yj->zxy', smooth, along_y, precision=lax.Precision.HIGHEST)
    depth_pos = jnp.arange(NZ, dtype=jnp.float32) / NZ
    row_pos = jnp.arange(NX, dtype=jnp.float32) / NX
    spread = 0.45 * (1.0 + 1.2 * row_pos[None, :, None] + 0.6 * depth_pos[:, None, None])
    jitter = jax.random.truncated_normal(noise_key, -2.5, 2.5, (NZ, NX, NY), jnp.float32)
    values = 0.6 * smooth + jitter * spread
    values = jnp.clip(values, -3.2, 3.2)
    return values.astype(jnp.float32)


def setup_inputs(seed: int = 0) -> dict:
    arg_keys = jax.random.split(jax.random.key(seed), 2)
    return {
        "concentration": draw_concentration(jax.random.fold_in(arg_keys[1], 71), 0),
    }


time_step = 100.0
kappa_grad = 2.0
stabilizer = 8.0


def wave_square(length):
    position = jnp.arange(length, dtype=jnp.int32)
    signed = jnp.where(2 * position >= length, position - length, position)
    phase_angle = signed.astype(jnp.float32) * (2.0 * math.pi / length)
    return phase_angle * phase_angle


def reference(concentration):
    squared = concentration * concentration
    bulk_sum = jnp.sum(0.25 * squared * squared - 0.5 * squared)
    cubic_term = squared * concentration - concentration
    spec_c = jnp.fft.fftn(concentration)
    spec_g = jnp.fft.fftn(cubic_term)
    wave_sq = wave_square(NZ)[:, None, None] + wave_square(NX)[None, :, None] + wave_square(NY)[None, None, :]
    numerator = 1.0 + time_step * stabilizer * wave_sq
    denominator = numerator + time_step * kappa_grad * wave_sq * wave_sq
    updated = (numerator * spec_c - time_step * wave_sq * spec_g) / denominator
    new_field = jnp.real(jnp.fft.ifftn(updated)).astype(jnp.float32)
    cell_count = NX * NY * NZ
    energy = (bulk_sum / cell_count).astype(jnp.float32)
    return (new_field, energy)
```

```python
import functools
import math

import jax
import jax.numpy as jnp
import numpy as np
from jax import lax
from jax.experimental import pallas as pl
from jax.experimental.pallas import tpu as pltpu
from jax.sharding import PartitionSpec as P

time_step = 100.0
kappa_grad = 2.0
stabilizer = 8.0
highest = lax.Precision.HIGHEST


def circle(length, first_total, second_total, direction):
    first_index = jnp.arange(first_total, dtype=jnp.int32)
    second_index = jnp.arange(second_total, dtype=jnp.int32)
    turn_index = first_index[:, None] * second_index[None, :] % length
    phase_angle = turn_index.astype(jnp.float32) * (2.0 * math.pi / length)
    return (jnp.cos(phase_angle), direction * jnp.sin(phase_angle))


def contract(pattern, real_part, imag_part, table_cos, table_sin):

    def product_of(operand, matrix):
        return jnp.einsum(pattern, operand, matrix, precision=highest)

    out_real = product_of(real_part, table_cos) - product_of(imag_part, table_sin)
    out_imag = product_of(real_part, table_sin) + product_of(imag_part, table_cos)
    return (out_real, out_imag)


def real_only(pattern, real_part, imag_part, table_cos, table_sin):
    return jnp.einsum(pattern, real_part, table_cos, precision=highest) - jnp.einsum(
        pattern, imag_part, table_sin, precision=highest
    )


def rotate(real_part, imag_part, table_cos, table_sin):
    return (
        real_part * table_cos - imag_part * table_sin,
        real_part * table_sin + imag_part * table_cos,
    )


def wave_square(storage, length, permuted):
    if permuted:
        actual = storage // 128 + length // 128 * (storage % 128)
    else:
        actual = storage
    signed = jnp.where(2 * actual >= length, actual - length, actual)
    phase_angle = signed.astype(jnp.float32) * (2.0 * math.pi / length)
    return phase_angle * phase_angle


def plain_step(concentration):
    plane_count, row_count, full_y = concentration.shape
    slab_count = lax.axis_size("slab")
    section_count = lax.axis_size("section")
    full_x = row_count * slab_count
    full_z = plane_count * section_count
    y_block = full_y // slab_count
    y_half = y_block // section_count
    blocks_x = full_x // 128
    blocks_y = full_y // 128
    cell_count = full_x * full_y * full_z
    slab_at = lax.axis_index("slab")
    section_at = lax.axis_index("section")
    squared = concentration * concentration
    bulk_sum = jnp.sum(0.25 * squared * squared - 0.5 * squared)
    cubic_term = squared * concentration - concentration
    shaped_c = concentration.reshape(1, plane_count, row_count, blocks_y, 128)
    shaped_g = cubic_term.reshape(1, plane_count, row_count, blocks_y, 128)
    first_cos, first_sin = circle(blocks_y, blocks_y, blocks_y, -1.0)
    part_real, part_imag = contract("fzxab,aj->fzxjb", shaped_c, shaped_g, first_cos, first_sin)
    field_total = part_real.shape[0]
    twist_cos, twist_sin = circle(full_y, blocks_y, 128, -1.0)
    part_real, part_imag = rotate(part_real, part_imag, twist_cos, twist_sin)
    lane_cos, lane_sin = circle(128, 128, 128, -1.0)
    part_real, part_imag = contract("fzxjb,bk->fxjkz", part_real, part_imag, lane_cos, lane_sin)
    outgoing = jnp.concatenate([part_real, part_imag], 0).reshape(
        2 * field_total, row_count, slab_count, y_block * plane_count
    )
    columns = lax.all_to_all(outgoing, "slab", split_axis=2, concat_axis=1, tiled=True)
    columns = columns.reshape(2 * field_total, blocks_x, 128, y_block * plane_count)
    first_cos, first_sin = circle(blocks_x, blocks_x, blocks_x, -1.0)
    part_real, part_imag = contract(
        "fabm,aj->fmjb", columns[:field_total], columns[field_total:], first_cos, first_sin
    )
    twist_cos, twist_sin = circle(full_x, blocks_x, 128, -1.0)
    part_real, part_imag = rotate(part_real, part_imag, twist_cos, twist_sin)
    part_real, part_imag = contract("fmjb,bk->fmjk", part_real, part_imag, lane_cos, lane_sin)
    spectra_x = jnp.concatenate([part_real, part_imag], 0).reshape(
        2 * field_total, y_block, plane_count, full_x
    )
    depth_cos, depth_sin = circle(full_z, full_z, full_z, -1.0)
    own_cos = lax.dynamic_slice_in_dim(depth_cos, section_at * plane_count, plane_count, 0)
    own_sin = lax.dynamic_slice_in_dim(depth_sin, section_at * plane_count, plane_count, 0)
    term_real, term_imag = contract(
        "fyzk,zq->yfqk", spectra_x[:field_total], spectra_x[field_total:], own_cos, own_sin
    )
    spectral = lax.psum_scatter(
        jnp.concatenate([term_real, term_imag], 1), "section", scatter_dimension=0, tiled=True
    )
    storage_y = slab_at * y_block + section_at * y_half + jnp.arange(y_half, dtype=jnp.int32)
    storage_x = jnp.arange(full_x, dtype=jnp.int32)
    storage_z = jnp.arange(full_z, dtype=jnp.int32)
    wave_sq = (
        wave_square(storage_y, full_y, True)[:, None, None]
        + wave_square(storage_z, full_z, False)[None, :, None]
        + wave_square(storage_x, full_x, True)[None, None, :]
    )
    numerator = 1.0 + time_step * stabilizer * wave_sq
    denominator = numerator + time_step * kappa_grad * wave_sq * wave_sq
    keep_rate = numerator / denominator
    mix_rate = time_step * wave_sq / denominator
    new_real = keep_rate * spectral[:, 0] - mix_rate * spectral[:, 1]
    new_imag = keep_rate * spectral[:, 1] + mix_rate * spectral[:, 0]
    back_cos, back_sin = circle(full_z, full_z, full_z, 1.0)
    part_real, part_imag = contract("yqk,qz->yzk", new_real, new_imag, back_cos, back_sin)
    returning = jnp.stack([part_real, part_imag], 1)
    own_planes = lax.all_to_all(returning, "section", split_axis=2, concat_axis=0, tiled=True)
    grid_real = own_planes[:, 0].reshape(y_block, plane_count, blocks_x, 128)
    grid_imag = own_planes[:, 1].reshape(y_block, plane_count, blocks_x, 128)
    lane_cos, lane_sin = circle(128, 128, 128, 1.0)
    part_real, part_imag = contract("szjk,kb->szjb", grid_real, grid_imag, lane_cos, lane_sin)
    twist_cos, twist_sin = circle(full_x, blocks_x, 128, 1.0)
    part_real, part_imag = rotate(part_real, part_imag, twist_cos, twist_sin)
    first_cos, first_sin = circle(blocks_x, blocks_x, blocks_x, 1.0)
    part_real, part_imag = contract("szjb,ja->absz", part_real, part_imag, first_cos, first_sin)
    leaving = jnp.stack([part_real, part_imag], 0).reshape(2, full_x, 1, y_block * plane_count)
    rows_back = lax.all_to_all(leaving, "slab", split_axis=1, concat_axis=2, tiled=True)
    rows_back = rows_back.reshape(2, row_count, blocks_y, 128, plane_count)
    part_real, part_imag = contract("xjkz,kb->xjbz", rows_back[0], rows_back[1], lane_cos, lane_sin)
    twist_cos, twist_sin = circle(full_y, blocks_y, 128, 1.0)
    part_real, part_imag = rotate(
        part_real, part_imag, twist_cos[:, :, None], twist_sin[:, :, None]
    )
    first_cos, first_sin = circle(blocks_y, blocks_y, blocks_y, 1.0)
    new_field = real_only("xjbz,ja->zxab", part_real, part_imag, first_cos, first_sin)
    new_field = new_field.reshape(plane_count, row_count, full_y) / cell_count
    total_bulk = lax.psum(bulk_sum, ("section", "slab"))
    energy = total_bulk / cell_count
    return (new_field, energy)


lanes = 128
row_group = 32
vmem_limit = 60 * 1024 * 1024


def split(values):
    high = values.astype(jnp.bfloat16)
    low = (values - high.astype(jnp.float32)).astype(jnp.bfloat16)
    return high, low


def triple(left_parts, right_parts, dims):
    def product(left, right):
        return lax.dot_general(left, right, (dims, ((), ())), preferred_element_type=jnp.float32)

    left_high, left_low = left_parts
    right_high, right_low = right_parts
    return (
        product(left_high, right_high)
        + product(left_low, right_high)
        + product(left_high, right_low)
    )


def y_tables(full_y, devices, parity):
    half = full_y // 2
    per_part = half // 2 // devices
    slot = np.arange(half)
    device, inner = slot // (2 * per_part), slot % (2 * per_part)
    part, local = inner // per_part, inner % per_part
    wave = parity + 2 * (device * per_part + local)
    position = np.arange(half)
    turns = wave[:, None] * position[None, :] % full_y
    phase = turns * (2.0 * math.pi / full_y)
    coarse = phase[::row_group]
    offset = wave[:row_group] - wave[0]
    fine = (offset[:, None] * position[None, :] % full_y) * (2.0 * math.pi / full_y)
    fine = fine + part[:row_group, None] * (0.5 * math.pi)
    return [
        table.astype(np.float32)
        for table in (np.cos(coarse), np.sin(coarse), np.cos(fine), np.sin(fine))
    ]


def y_block(refs, block, groups, parity):
    coarse_cos, coarse_sin, fine_cos, fine_sin = refs
    cos_fine, sin_fine = fine_cos[...], fine_sin[...]
    width = cos_fine.shape[1]
    pieces = []
    for group in range(block * groups, (block + 1) * groups):
        piece = coarse_cos[group : group + 1, :] * cos_fine - coarse_sin[group : group + 1, :] * sin_fine
        if parity == 0 and group == 0:
            row = lax.broadcasted_iota(jnp.int32, piece.shape, 0)
            column = lax.broadcasted_iota(jnp.int32, piece.shape, 1)
            sign = 1.0 - 2.0 * (column % 2).astype(jnp.float32)
            piece = jnp.where(row == row_group // 2, sign, piece)
        pieces.append(piece)
    return jnp.concatenate(pieces, 0)


def forward_kernel(parity, conc_ref, ta, tb, tc, td, out_ref, high_ref, low_ref):
    planes, rows, full_y = conc_ref.shape
    half = full_y // 2
    for plane in range(planes):
        first = conc_ref[plane, :, :half]
        second = conc_ref[plane, :, half:]
        first_g = first * first * first - first
        second_g = second * second * second - second
        for field, (left, right) in enumerate(((first, second), (first_g, second_g))):
            mixed = left + right if parity == 0 else left - right
            high, low = split(mixed)
            at = (plane * 2 + field) * rows
            high_ref[at : at + rows, :] = high
            low_ref[at : at + rows, :] = low
    groups = 8
    for block in range(half // (groups * row_group)):
        table = y_block((ta, tb, tc, td), block, groups, parity)
        result = triple(split(table), (high_ref[...], low_ref[...]), ((1,), (1,)))
        out_ref[block * groups : (block + 1) * groups] = result.reshape(groups, row_group, -1)


def backward_part(parity, in_ref, tables):
    devices, inner, columns = in_ref.shape
    groups = 8
    total = None
    for block in range(devices // groups):
        rows = in_ref[block * groups : (block + 1) * groups].reshape(groups * inner, columns)
        table = y_block(tables, block, groups, parity)
        term = triple(split(rows.T), split(table), ((1,), (0,)))
        total = term if total is None else total + term
    return total


def backward_even_kernel(in_ref, ta, tb, tc, td, out_ref):
    out_ref[...] = backward_part(0, in_ref, (ta, tb, tc, td))


def backward_odd_kernel(in_ref, even_ref, ta, tb, tc, td, out_ref):
    planes, rows, full_y = out_ref.shape
    half = full_y // 2
    odd = backward_part(1, in_ref, (ta, tb, tc, td))
    for plane in range(planes):
        even_rows = even_ref[plane * rows : (plane + 1) * rows, :]
        odd_rows = odd[plane * rows : (plane + 1) * rows, :]
        out_ref[plane, :, :half] = even_rows + odd_rows
        out_ref[plane, :, half:] = even_rows - odd_rows


def times_unit(real, imag, quarter_turns):
    turns = quarter_turns % 4
    if turns == 0:
        return real, imag
    if turns == 1:
        return -imag, real
    if turns == 2:
        return -real, -imag
    return imag, -real


def unit_sum(parts, power, direction):
    total_real, total_imag = parts[0]
    for index in range(1, len(parts)):
        real, imag = times_unit(*parts[index], direction * power * index)
        total_real = total_real + real
        total_imag = total_imag + imag
    return total_real, total_imag


def middle_kernel(
    has_extra, sections, in_ref, aux_ref, wx_ref, tw_cos, tw_sin, high_ref, low_ref, out_ref,
    spec_ref, fil_ref, back_ref,
):
    devices, inner, columns = in_ref.shape
    kk = inner // 2
    slabs = devices // sections
    zf_local = columns // lanes
    planes = zf_local // 2
    full_z = planes * sections
    quarter = slabs // 4
    width = quarter * lanes
    padded = spec_ref.shape[3]
    special = aux_ref[2, 0:8, 0:1] if has_extra else None

    def gather(section, a, part, row, zf):
        pieces = [
            in_ref[
                section * slabs + a * quarter + step,
                part * kk + row : part * kk + row + 8,
                zf * lanes : (zf + 1) * lanes,
            ]
            for step in range(quarter)
        ]
        return jnp.concatenate(pieces, 1)

    for section in range(sections):
        for zf in range(zf_local):
            at = section * zf_local + zf
            for row in range(0, padded, 8):
                source = 0 if row >= kk else row
                parts = []
                for a in range(4):
                    imag = gather(section, a, 1, source, zf)
                    if row >= kk:
                        real, imag = imag * special, jnp.zeros_like(imag)
                    else:
                        real = gather(section, a, 0, source, zf)
                        if has_extra and row == 0:
                            imag = imag * (1.0 - special)
                    parts.append((real, imag))
                for j in range(4):
                    real, imag = unit_sum(parts, j, -1)
                    if j:
                        cos, sin = tw_cos[j : j + 1, :], tw_sin[j : j + 1, :]
                        real, imag = real * cos + imag * sin, imag * cos - real * sin
                    spec_ref[j, 0, at, row : row + 8, :] = real
                    spec_ref[j, 1, at, row : row + 8, :] = imag

    weights = (high_ref[...], low_ref[...])
    total_zf = sections * zf_local
    for j in range(4):
        rows = spec_ref[j].reshape(2 * total_zf * padded, width)
        raw = triple(split(rows), weights, ((1,), (0,)))
        raw = raw.reshape(2, total_zf, padded, 2 * width)
        for row in range(0, padded, 8):
            fields = []
            for field in range(2):
                per_z = []
                for z in range(full_z):
                    at = z * 2 + field
                    re_part = raw[0, at, row : row + 8]
                    im_part = raw[1, at, row : row + 8]
                    per_z.append(
                        (
                            re_part[:, :width] + im_part[:, width:],
                            im_part[:, :width] - re_part[:, width:],
                        )
                    )
                fields.append(per_z)
            plane_sq = aux_ref[0, row : row + 8, 0:1] + wx_ref[j : j + 1, :]
            weight = aux_ref[1, row : row + 8, 0:1]
            updated = []
            for q in range(full_z):
                c_real, c_imag = unit_sum(fields[0], q, -1)
                g_real, g_imag = unit_sum(fields[1], q, -1)
                signed = q - full_z if 2 * q >= full_z else q
                wave_sq = plane_sq + (2.0 * math.pi * signed / full_z) ** 2
                numerator = 1.0 + time_step * stabilizer * wave_sq
                denominator = numerator + time_step * kappa_grad * wave_sq * wave_sq
                inverse = weight / denominator
                keep = numerator * inverse
                mix = time_step * wave_sq * inverse
                updated.append((keep * c_real - mix * g_real, keep * c_imag - mix * g_imag))
            for z in range(full_z):
                real, imag = unit_sum(updated, z, 1)
                fil_ref[0, z, row : row + 8, :] = real
                fil_ref[1, z, row : row + 8, :] = imag
        rows = fil_ref[...].reshape(2 * full_z * padded, width)
        raw = triple(split(rows), weights, ((1,), (0,)))
        raw = raw.reshape(2, full_z, padded, 2 * width)
        real = raw[0, :, :, :width] - raw[1, :, :, width:]
        imag = raw[0, :, :, width:] + raw[1, :, :, :width]
        cos, sin = tw_cos[j : j + 1, :], tw_sin[j : j + 1, :]
        back_ref[j, 0] = real * cos - imag * sin
        back_ref[j, 1] = imag * cos + real * sin

    for z in range(full_z):
        section, plane = z // planes, z % planes
        for row in range(0, kk, 8):
            parts = [
                (back_ref[j, 0, z, row : row + 8, :], back_ref[j, 1, z, row : row + 8, :])
                for j in range(4)
            ]
            extra = None
            if has_extra and row == 0:
                extra = [
                    (back_ref[j, 0, z, kk : kk + 8, :], back_ref[j, 1, z, kk : kk + 8, :])
                    for j in range(4)
                ]
            for a in range(4):
                real, imag = unit_sum(parts, a, 1)
                if extra is not None:
                    extra_real, _ = unit_sum(extra, a, 1)
                    imag = imag * (1.0 - special) + extra_real * special
                for step in range(quarter):
                    target = section * slabs + a * quarter + step
                    piece = slice(step * lanes, (step + 1) * lanes)
                    column = slice(plane * lanes, (plane + 1) * lanes)
                    out_ref[target, row : row + 8, column] = real[:, piece]
                    out_ref[target, kk + row : kk + row + 8, column] = imag[:, piece]


def kernel_call(body, out_shape, scratch, flops, moved, *operands):
    return pl.pallas_call(
        body,
        out_shape=jax.ShapeDtypeStruct(out_shape, jnp.float32),
        in_specs=[pl.BlockSpec(memory_space=pltpu.VMEM)] * len(operands),
        out_specs=pl.BlockSpec(memory_space=pltpu.VMEM),
        scratch_shapes=scratch,
        compiler_params=pltpu.CompilerParams(vmem_limit_bytes=vmem_limit),
        cost_estimate=pl.CostEstimate(flops=flops, bytes_accessed=moved, transcendentals=0),
    )(*operands)


def signed_square(index, length):
    signed = jnp.where(2 * index >= length, index - length, index)
    angle = signed.astype(jnp.float32) * (2.0 * math.pi / length)
    return angle * angle


def kernel_step(concentration):
    planes, rows, full_y = concentration.shape
    slabs = lax.axis_size("slab")
    sections = lax.axis_size("section")
    devices = slabs * sections
    full_x = rows * slabs
    full_z = planes * sections
    cells = full_x * full_y * full_z
    half = full_y // 2
    kk = half // 2 // devices
    width = full_x // 4
    me = lax.axis_index("section") * slabs + lax.axis_index("slab")
    axes = ("section", "slab")
    base = np.arange(width)
    turn = (base[:, None] * base[None, :] % width) * (2.0 * math.pi / width)
    dft = np.concatenate([np.cos(turn), np.sin(turn)], 1).astype(np.float32)
    dft_high = dft.astype(jnp.bfloat16)
    dft_low = (dft - dft_high.astype(np.float32)).astype(jnp.bfloat16)
    twist = np.arange(4)[:, None] * base[None, :] * (2.0 * math.pi / full_x)
    twist_cos, twist_sin = np.cos(twist).astype(np.float32), np.sin(twist).astype(np.float32)
    kx = np.arange(4)[:, None] + 4 * base[None, :]
    kx = np.where(2 * kx >= full_x, kx - full_x, kx) * (2.0 * math.pi / full_x)
    wave_x = (kx * kx).astype(np.float32)
    tables = [y_tables(full_y, devices, parity) for parity in range(2)]
    columns = planes * 2 * rows
    flops = 6 * half * half * columns
    arrived = []
    for parity in range(2):
        sent = kernel_call(
            functools.partial(forward_kernel, parity),
            (devices, 2 * kk, columns),
            [pltpu.VMEM((columns, half), jnp.bfloat16)] * 2,
            flops,
            4 * concentration.size + 4 * half * columns,
            concentration,
            *tables[parity],
        )
        arrived.append(lax.all_to_all(sent, axes, split_axis=0, concat_axis=0, tiled=True))
    returned = []
    for parity in range(2):
        has_extra = parity == 0
        padded = kk + 8 if has_extra else kk
        row = jnp.arange(padded, dtype=jnp.int32)
        wave = parity + 2 * (me * kk + row)
        extra_row = row >= kk
        if has_extra:
            wave = jnp.where(extra_row, half, wave)
        first = (wave == 0) | extra_row
        weight = jnp.where(first, 1.0 / cells, 2.0 / cells)
        flag = jnp.where((row == 0) & (me == 0), 1.0, 0.0)
        aux = jnp.stack([signed_square(wave, full_y), weight, flag]).astype(jnp.float32)
        aux = jnp.broadcast_to(aux[:, :, None], (3, padded, lanes))
        sent = kernel_call(
            functools.partial(middle_kernel, has_extra, sections),
            (devices, 2 * kk, planes * rows),
            [
                pltpu.VMEM((4, 2, 2 * full_z, padded, width), jnp.float32),
                pltpu.VMEM((2, full_z, padded, width), jnp.float32),
                pltpu.VMEM((4, 2, full_z, padded, width), jnp.float32),
            ],
            6 * 24 * full_z * padded * width * 2 * width,
            4 * half * columns,
            arrived[parity],
            aux,
            wave_x,
            twist_cos,
            twist_sin,
            dft_high,
            dft_low,
        )
        returned.append(lax.all_to_all(sent, axes, split_axis=0, concat_axis=0, tiled=True))
    even = kernel_call(
        backward_even_kernel,
        (planes * rows, half),
        [],
        flops // 2,
        8 * half * columns,
        returned[0],
        *tables[0],
    )
    new_field = kernel_call(
        backward_odd_kernel,
        concentration.shape,
        [],
        flops // 2,
        8 * half * columns,
        returned[1],
        even,
        *tables[1],
    )
    squared = concentration * concentration
    bulk_sum = jnp.sum(0.25 * squared * squared - 0.5 * squared)
    energy = lax.psum(bulk_sum, axes) / cells
    return (new_field, energy)


def per_device(concentration):
    planes, rows, full_y = concentration.shape
    devices = lax.axis_size("slab") * lax.axis_size("section")
    share = full_y // 4 // devices
    fits = (
        rows == lanes
        and planes * lax.axis_size("section") == 4
        and 2 * share == row_group
        and devices % 8 == 0
        and lax.axis_size("slab") % 4 == 0
    )
    return kernel_step(concentration) if fits else plain_step(concentration)


def solution(mesh):
    return jax.shard_map(
        per_device,
        mesh=mesh,
        in_specs=(P("section", "slab", None),),
        out_specs=(P("section", "slab", None), P()),
        check_vma=False,
    )
```

```python
import functools
import math

import jax
import jax.numpy as jnp
import numpy as np
from jax import lax
from jax.experimental import pallas as pl
from jax.experimental.pallas import tpu as pltpu
from jax.sharding import PartitionSpec as P

time_step = 100.0
kappa_grad = 2.0
stabilizer = 8.0
highest = lax.Precision.HIGHEST


def circle(length, first_total, second_total, direction):
    first_index = jnp.arange(first_total, dtype=jnp.int32)
    second_index = jnp.arange(second_total, dtype=jnp.int32)
    turn_index = first_index[:, None] * second_index[None, :] % length
    phase_angle = turn_index.astype(jnp.float32) * (2.0 * math.pi / length)
    return (jnp.cos(phase_angle), direction * jnp.sin(phase_angle))


def contract(pattern, real_part, imag_part, table_cos, table_sin):

    def product_of(operand, matrix):
        return jnp.einsum(pattern, operand, matrix, precision=highest)

    out_real = product_of(real_part, table_cos) - product_of(imag_part, table_sin)
    out_imag = product_of(real_part, table_sin) + product_of(imag_part, table_cos)
    return (out_real, out_imag)


def real_only(pattern, real_part, imag_part, table_cos, table_sin):
    return jnp.einsum(pattern, real_part, table_cos, precision=highest) - jnp.einsum(
        pattern, imag_part, table_sin, precision=highest
    )


def rotate(real_part, imag_part, table_cos, table_sin):
    return (
        real_part * table_cos - imag_part * table_sin,
        real_part * table_sin + imag_part * table_cos,
    )


def wave_square(storage, length, permuted):
    if permuted:
        actual = storage // 128 + length // 128 * (storage % 128)
    else:
        actual = storage
    signed = jnp.where(2 * actual >= length, actual - length, actual)
    phase_angle = signed.astype(jnp.float32) * (2.0 * math.pi / length)
    return phase_angle * phase_angle


def plain_step(concentration):
    plane_count, row_count, full_y = concentration.shape
    slab_count = lax.axis_size("slab")
    section_count = lax.axis_size("section")
    full_x = row_count * slab_count
    full_z = plane_count * section_count
    y_block = full_y // slab_count
    y_half = y_block // section_count
    blocks_x = full_x // 128
    blocks_y = full_y // 128
    cell_count = full_x * full_y * full_z
    slab_at = lax.axis_index("slab")
    section_at = lax.axis_index("section")
    squared = concentration * concentration
    bulk_sum = jnp.sum(0.25 * squared * squared - 0.5 * squared)
    cubic_term = squared * concentration - concentration
    shaped_c = concentration.reshape(1, plane_count, row_count, blocks_y, 128)
    shaped_g = cubic_term.reshape(1, plane_count, row_count, blocks_y, 128)
    first_cos, first_sin = circle(blocks_y, blocks_y, blocks_y, -1.0)
    part_real, part_imag = contract("fzxab,aj->fzxjb", shaped_c, shaped_g, first_cos, first_sin)
    field_total = part_real.shape[0]
    twist_cos, twist_sin = circle(full_y, blocks_y, 128, -1.0)
    part_real, part_imag = rotate(part_real, part_imag, twist_cos, twist_sin)
    lane_cos, lane_sin = circle(128, 128, 128, -1.0)
    part_real, part_imag = contract("fzxjb,bk->fxjkz", part_real, part_imag, lane_cos, lane_sin)
    outgoing = jnp.concatenate([part_real, part_imag], 0).reshape(
        2 * field_total, row_count, slab_count, y_block * plane_count
    )
    columns = lax.all_to_all(outgoing, "slab", split_axis=2, concat_axis=1, tiled=True)
    columns = columns.reshape(2 * field_total, blocks_x, 128, y_block * plane_count)
    first_cos, first_sin = circle(blocks_x, blocks_x, blocks_x, -1.0)
    part_real, part_imag = contract(
        "fabm,aj->fmjb", columns[:field_total], columns[field_total:], first_cos, first_sin
    )
    twist_cos, twist_sin = circle(full_x, blocks_x, 128, -1.0)
    part_real, part_imag = rotate(part_real, part_imag, twist_cos, twist_sin)
    part_real, part_imag = contract("fmjb,bk->fmjk", part_real, part_imag, lane_cos, lane_sin)
    spectra_x = jnp.concatenate([part_real, part_imag], 0).reshape(
        2 * field_total, y_block, plane_count, full_x
    )
    depth_cos, depth_sin = circle(full_z, full_z, full_z, -1.0)
    own_cos = lax.dynamic_slice_in_dim(depth_cos, section_at * plane_count, plane_count, 0)
    own_sin = lax.dynamic_slice_in_dim(depth_sin, section_at * plane_count, plane_count, 0)
    term_real, term_imag = contract(
        "fyzk,zq->yfqk", spectra_x[:field_total], spectra_x[field_total:], own_cos, own_sin
    )
    spectral = lax.psum_scatter(
        jnp.concatenate([term_real, term_imag], 1), "section", scatter_dimension=0, tiled=True
    )
    storage_y = slab_at * y_block + section_at * y_half + jnp.arange(y_half, dtype=jnp.int32)
    storage_x = jnp.arange(full_x, dtype=jnp.int32)
    storage_z = jnp.arange(full_z, dtype=jnp.int32)
    wave_sq = (
        wave_square(storage_y, full_y, True)[:, None, None]
        + wave_square(storage_z, full_z, False)[None, :, None]
        + wave_square(storage_x, full_x, True)[None, None, :]
    )
    numerator = 1.0 + time_step * stabilizer * wave_sq
    denominator = numerator + time_step * kappa_grad * wave_sq * wave_sq
    keep_rate = numerator / denominator
    mix_rate = time_step * wave_sq / denominator
    new_real = keep_rate * spectral[:, 0] - mix_rate * spectral[:, 1]
    new_imag = keep_rate * spectral[:, 1] + mix_rate * spectral[:, 0]
    back_cos, back_sin = circle(full_z, full_z, full_z, 1.0)
    part_real, part_imag = contract("yqk,qz->yzk", new_real, new_imag, back_cos, back_sin)
    returning = jnp.stack([part_real, part_imag], 1)
    own_planes = lax.all_to_all(returning, "section", split_axis=2, concat_axis=0, tiled=True)
    grid_real = own_planes[:, 0].reshape(y_block, plane_count, blocks_x, 128)
    grid_imag = own_planes[:, 1].reshape(y_block, plane_count, blocks_x, 128)
    lane_cos, lane_sin = circle(128, 128, 128, 1.0)
    part_real, part_imag = contract("szjk,kb->szjb", grid_real, grid_imag, lane_cos, lane_sin)
    twist_cos, twist_sin = circle(full_x, blocks_x, 128, 1.0)
    part_real, part_imag = rotate(part_real, part_imag, twist_cos, twist_sin)
    first_cos, first_sin = circle(blocks_x, blocks_x, blocks_x, 1.0)
    part_real, part_imag = contract("szjb,ja->absz", part_real, part_imag, first_cos, first_sin)
    leaving = jnp.stack([part_real, part_imag], 0).reshape(2, full_x, 1, y_block * plane_count)
    rows_back = lax.all_to_all(leaving, "slab", split_axis=1, concat_axis=2, tiled=True)
    rows_back = rows_back.reshape(2, row_count, blocks_y, 128, plane_count)
    part_real, part_imag = contract("xjkz,kb->xjbz", rows_back[0], rows_back[1], lane_cos, lane_sin)
    twist_cos, twist_sin = circle(full_y, blocks_y, 128, 1.0)
    part_real, part_imag = rotate(
        part_real, part_imag, twist_cos[:, :, None], twist_sin[:, :, None]
    )
    first_cos, first_sin = circle(blocks_y, blocks_y, blocks_y, 1.0)
    new_field = real_only("xjbz,ja->zxab", part_real, part_imag, first_cos, first_sin)
    new_field = new_field.reshape(plane_count, row_count, full_y) / cell_count
    total_bulk = lax.psum(bulk_sum, ("section", "slab"))
    energy = total_bulk / cell_count
    return (new_field, energy)


lanes = 128
row_group = 32
vmem_limit = 60 * 1024 * 1024


def split(values):
    high = values.astype(jnp.bfloat16)
    low = (values - high.astype(jnp.float32)).astype(jnp.bfloat16)
    return high, low


def triple(left_parts, right_parts, dims):
    def product(left, right):
        return lax.dot_general(left, right, (dims, ((), ())), preferred_element_type=jnp.float32)

    left_high, left_low = left_parts
    right_high, right_low = right_parts
    return (
        product(left_high, right_high)
        + product(left_low, right_high)
        + product(left_high, right_low)
    )


def y_tables(full_y, devices, parity):
    half = full_y // 2
    per_part = half // 2 // devices
    slot = np.arange(half)
    device, inner = slot // (2 * per_part), slot % (2 * per_part)
    part, local = inner // per_part, inner % per_part
    wave = parity + 2 * (device * per_part + local)
    position = np.arange(half)
    turns = wave[:, None] * position[None, :] % full_y
    phase = turns * (2.0 * math.pi / full_y)
    coarse = phase[::row_group]
    offset = wave[:row_group] - wave[0]
    fine = (offset[:, None] * position[None, :] % full_y) * (2.0 * math.pi / full_y)
    fine = fine + part[:row_group, None] * (0.5 * math.pi)
    return [
        table.astype(np.float32)
        for table in (np.cos(coarse), np.sin(coarse), np.cos(fine), np.sin(fine))
    ]


def y_block(refs, block, groups, parity):
    coarse_cos, coarse_sin, fine_cos, fine_sin = refs
    cos_fine, sin_fine = fine_cos[...], fine_sin[...]
    width = cos_fine.shape[1]
    pieces = []
    for group in range(block * groups, (block + 1) * groups):
        piece = coarse_cos[group : group + 1, :] * cos_fine - coarse_sin[group : group + 1, :] * sin_fine
        if parity == 0 and group == 0:
            row = lax.broadcasted_iota(jnp.int32, piece.shape, 0)
            column = lax.broadcasted_iota(jnp.int32, piece.shape, 1)
            sign = 1.0 - 2.0 * (column % 2).astype(jnp.float32)
            piece = jnp.where(row == row_group // 2, sign, piece)
        pieces.append(piece)
    return jnp.concatenate(pieces, 0)


def forward_kernel(parity, conc_ref, ta, tb, tc, td, out_ref, high_ref, low_ref):
    planes, rows, full_y = conc_ref.shape
    half = full_y // 2
    for plane in range(planes):
        first = conc_ref[plane, :, :half]
        second = conc_ref[plane, :, half:]
        first_g = first * first * first - first
        second_g = second * second * second - second
        for field, (left, right) in enumerate(((first, second), (first_g, second_g))):
            mixed = left + right if parity == 0 else left - right
            high, low = split(mixed)
            at = (plane * 2 + field) * rows
            high_ref[at : at + rows, :] = high
            low_ref[at : at + rows, :] = low
    groups = 8
    for block in range(half // (groups * row_group)):
        table = y_block((ta, tb, tc, td), block, groups, parity)
        result = triple(split(table), (high_ref[...], low_ref[...]), ((1,), (1,)))
        out_ref[block * groups : (block + 1) * groups] = result.reshape(groups, row_group, -1)


def backward_part(parity, in_ref, tables):
    devices, inner, columns = in_ref.shape
    groups = 8
    total = None
    for block in range(devices // groups):
        at = slice(block * groups, (block + 1) * groups)
        turned = [
            in_ref[at, plane * row_group : (plane + 1) * row_group, :]
            .reshape(groups * row_group, columns)
            .T
            for plane in range(inner // row_group)
        ]
        table = y_block(tables, block, groups, parity)
        term = triple(split(jnp.concatenate(turned, 0)), split(table), ((1,), (0,)))
        total = term if total is None else total + term
    return total


def backward_even_kernel(in_ref, ta, tb, tc, td, out_ref):
    out_ref[...] = backward_part(0, in_ref, (ta, tb, tc, td))


def backward_odd_kernel(in_ref, even_ref, ta, tb, tc, td, out_ref):
    planes, rows, full_y = out_ref.shape
    half = full_y // 2
    odd = backward_part(1, in_ref, (ta, tb, tc, td))
    for plane in range(planes):
        even_rows = even_ref[plane * rows : (plane + 1) * rows, :]
        odd_rows = odd[plane * rows : (plane + 1) * rows, :]
        out_ref[plane, :, :half] = even_rows + odd_rows
        out_ref[plane, :, half:] = even_rows - odd_rows


def times_unit(real, imag, quarter_turns):
    turns = quarter_turns % 4
    if turns == 0:
        return real, imag
    if turns == 1:
        return -imag, real
    if turns == 2:
        return -real, -imag
    return imag, -real


def unit_sum(parts, power, direction):
    total_real, total_imag = parts[0]
    for index in range(1, len(parts)):
        real, imag = times_unit(*parts[index], direction * power * index)
        total_real = total_real + real
        total_imag = total_imag + imag
    return total_real, total_imag


def middle_kernel(
    has_extra, sections, in_ref, aux_ref, wx_ref, tw_cos, tw_sin, ca, sa, cb, sb, *rest
):
    if has_extra:
        part_ref, out_ref, spec_ref, fil_ref, back_ref = rest
    else:
        out_ref, spec_ref, fil_ref, back_ref = rest
    devices, inner, columns = in_ref.shape
    kk = inner // 2
    slabs = devices // sections
    zf_local = columns // lanes
    planes = zf_local // 2
    full_z = planes * sections
    quarter = slabs // 4
    width = quarter * lanes
    padded = spec_ref.shape[3]
    special = aux_ref[2, 0:8, 0:1] if has_extra else None

    def gather(section, a, part, row, zf):
        pieces = [
            in_ref[
                section * slabs + a * quarter + step,
                part * kk + row : part * kk + row + 8,
                zf * lanes : (zf + 1) * lanes,
            ]
            for step in range(quarter)
        ]
        return jnp.concatenate(pieces, 1)

    for section in range(sections):
        for zf in range(zf_local):
            at = section * zf_local + zf
            for row in range(0, padded, 8):
                source = 0 if row >= kk else row
                parts = []
                for a in range(4):
                    imag = gather(section, a, 1, source, zf)
                    if row >= kk:
                        real, imag = imag * special, jnp.zeros_like(imag)
                    else:
                        real = gather(section, a, 0, source, zf)
                        if has_extra and row == 0:
                            imag = imag * (1.0 - special)
                    parts.append((real, imag))
                for j in range(4):
                    real, imag = unit_sum(parts, j, -1)
                    if j:
                        cos, sin = tw_cos[j : j + 1, :], tw_sin[j : j + 1, :]
                        real, imag = real * cos + imag * sin, imag * cos - real * sin
                    spec_ref[j, 0, at, row : row + 8, :] = real
                    spec_ref[j, 1, at, row : row + 8, :] = imag

    cos_rows, sin_rows = [], []
    cos_fine, sin_fine = cb[...], sb[...]
    for group in range(ca.shape[0]):
        cos_base, sin_base = ca[group : group + 1, :], sa[group : group + 1, :]
        cos_rows.append(cos_base * cos_fine - sin_base * sin_fine)
        sin_rows.append(sin_base * cos_fine + cos_base * sin_fine)
    table = jnp.concatenate([jnp.concatenate(cos_rows, 0), jnp.concatenate(sin_rows, 0)], 1)
    weights = split(table)
    total_zf = sections * zf_local
    for j in range(4):
        rows = spec_ref[j].reshape(2 * total_zf * padded, width)
        raw = triple(split(rows), weights, ((1,), (0,)))
        raw = raw.reshape(2, total_zf, padded, 2 * width)
        for row in range(0, padded, 8):
            fields = []
            for field in range(2):
                per_z = []
                for z in range(full_z):
                    at = z * 2 + field
                    re_part = raw[0, at, row : row + 8]
                    im_part = raw[1, at, row : row + 8]
                    per_z.append(
                        (
                            re_part[:, :width] + im_part[:, width:],
                            im_part[:, :width] - re_part[:, width:],
                        )
                    )
                fields.append(per_z)
            plane_sq = aux_ref[0, row : row + 8, 0:1] + wx_ref[j : j + 1, :]
            weight = aux_ref[1, row : row + 8, 0:1]
            updated = []
            for q in range(full_z):
                c_real, c_imag = unit_sum(fields[0], q, -1)
                g_real, g_imag = unit_sum(fields[1], q, -1)
                signed = q - full_z if 2 * q >= full_z else q
                wave_sq = plane_sq + (2.0 * math.pi * signed / full_z) ** 2
                numerator = 1.0 + time_step * stabilizer * wave_sq
                denominator = numerator + time_step * kappa_grad * wave_sq * wave_sq
                inverse = weight / denominator
                keep = numerator * inverse
                mix = time_step * wave_sq * inverse
                updated.append((keep * c_real - mix * g_real, keep * c_imag - mix * g_imag))
            for z in range(full_z):
                real, imag = unit_sum(updated, z, 1)
                fil_ref[0, z, row : row + 8, :] = real
                fil_ref[1, z, row : row + 8, :] = imag
        rows = fil_ref[...].reshape(2 * full_z * padded, width)
        raw = triple(split(rows), weights, ((1,), (0,)))
        raw = raw.reshape(2, full_z, padded, 2 * width)
        real = raw[0, :, :, :width] - raw[1, :, :, width:]
        imag = raw[0, :, :, width:] + raw[1, :, :, :width]
        cos, sin = tw_cos[j : j + 1, :], tw_sin[j : j + 1, :]
        back_ref[j, 0] = real * cos - imag * sin
        back_ref[j, 1] = imag * cos + real * sin

    for z in range(full_z):
        section, plane = z // planes, z % planes
        for row in range(0, kk, 8):
            parts = [
                (back_ref[j, 0, z, row : row + 8, :], back_ref[j, 1, z, row : row + 8, :])
                for j in range(4)
            ]
            extra = None
            if has_extra and row == 0:
                extra = [
                    (back_ref[j, 0, z, kk : kk + 8, :], back_ref[j, 1, z, kk : kk + 8, :])
                    for j in range(4)
                ]
            for a in range(4):
                real, imag = unit_sum(parts, a, 1)
                if extra is not None:
                    extra_real, _ = unit_sum(extra, a, 1)
                    imag = imag * (1.0 - special) + extra_real * special
                for step in range(quarter):
                    target = section * slabs + a * quarter + step
                    piece = slice(step * lanes, (step + 1) * lanes)
                    at = plane * inner + row
                    out_ref[target, at : at + 8, :] = real[:, piece]
                    out_ref[target, at + kk : at + kk + 8, :] = imag[:, piece]
    if has_extra:
        for target in range(devices):
            out_ref[target, planes * inner :, :] = part_ref[...]


def kernel_call(body, out_shape, scratch, flops, moved, *operands):
    return pl.pallas_call(
        body,
        out_shape=jax.ShapeDtypeStruct(out_shape, jnp.float32),
        in_specs=[pl.BlockSpec(memory_space=pltpu.VMEM)] * len(operands),
        out_specs=pl.BlockSpec(memory_space=pltpu.VMEM),
        scratch_shapes=scratch,
        compiler_params=pltpu.CompilerParams(vmem_limit_bytes=vmem_limit),
        cost_estimate=pl.CostEstimate(flops=flops, bytes_accessed=moved, transcendentals=0),
    )(*operands)


def signed_square(index, length):
    signed = jnp.where(2 * index >= length, index - length, index)
    angle = signed.astype(jnp.float32) * (2.0 * math.pi / length)
    return angle * angle


def kernel_step(concentration):
    planes, rows, full_y = concentration.shape
    slabs = lax.axis_size("slab")
    sections = lax.axis_size("section")
    devices = slabs * sections
    full_x = rows * slabs
    full_z = planes * sections
    cells = full_x * full_y * full_z
    half = full_y // 2
    kk = half // 2 // devices
    width = full_x // 4
    me = lax.axis_index("section") * slabs + lax.axis_index("slab")
    axes = ("section", "slab")
    base = np.arange(width)
    step = 2.0 * math.pi / width
    coarse = base[::row_group, None] * base[None, :] % width * step
    fine = base[:row_group, None] * base[None, :] % width * step
    dft = [f(t).astype(np.float32) for t in (coarse, fine) for f in (np.cos, np.sin)]
    twist = np.arange(4)[:, None] * base[None, :] * (2.0 * math.pi / full_x)
    twist_cos, twist_sin = np.cos(twist).astype(np.float32), np.sin(twist).astype(np.float32)
    kx = np.arange(4)[:, None] + 4 * base[None, :]
    kx = np.where(2 * kx >= full_x, kx - full_x, kx) * (2.0 * math.pi / full_x)
    wave_x = (kx * kx).astype(np.float32)
    tables = [y_tables(full_y, devices, parity) for parity in range(2)]
    columns = planes * 2 * rows
    flops = 6 * half * half * columns
    squared = concentration * concentration
    bulk_sum = jnp.sum(0.25 * squared * squared - 0.5 * squared)
    arrived = []
    for parity in range(2):
        sent = kernel_call(
            functools.partial(forward_kernel, parity),
            (devices, 2 * kk, columns),
            [pltpu.VMEM((columns, half), jnp.bfloat16)] * 2,
            flops,
            4 * concentration.size + 4 * half * columns,
            concentration,
            *tables[parity],
        )
        arrived.append(lax.all_to_all(sent, axes, split_axis=0, concat_axis=0, tiled=True))
    returned = []
    for parity in range(2):
        has_extra = parity == 0
        padded = kk + 8 if has_extra else kk
        row = jnp.arange(padded, dtype=jnp.int32)
        wave = parity + 2 * (me * kk + row)
        extra_row = row >= kk
        if has_extra:
            wave = jnp.where(extra_row, half, wave)
        first = (wave == 0) | extra_row
        weight = jnp.where(first, 1.0 / cells, 2.0 / cells)
        flag = jnp.where((row == 0) & (me == 0), 1.0, 0.0)
        aux = jnp.stack([signed_square(wave, full_y), weight, flag]).astype(jnp.float32)
        aux = jnp.broadcast_to(aux[:, :, None], (3, padded, lanes))
        sent = kernel_call(
            functools.partial(middle_kernel, has_extra, sections),
            (devices, 2 * kk * planes + (8 if has_extra else 0), rows),
            [
                pltpu.VMEM((4, 2, 2 * full_z, padded, width), jnp.float32),
                pltpu.VMEM((2, full_z, padded, width), jnp.float32),
                pltpu.VMEM((4, 2, full_z, padded, width), jnp.float32),
            ],
            6 * 24 * full_z * padded * width * 2 * width,
            4 * half * columns,
            arrived[parity],
            aux,
            wave_x,
            twist_cos,
            twist_sin,
            *dft,
            *([jnp.full((8, lanes), bulk_sum)] if has_extra else []),
        )
        returned.append(lax.all_to_all(sent, axes, split_axis=0, concat_axis=0, tiled=True))
    even = kernel_call(
        backward_even_kernel,
        (planes * rows, half),
        [],
        flops // 2,
        8 * half * columns,
        returned[0],
        *tables[0],
    )
    new_field = kernel_call(
        backward_odd_kernel,
        concentration.shape,
        [],
        flops // 2,
        8 * half * columns,
        returned[1],
        even,
        *tables[1],
    )
    energy = jnp.sum(returned[0][:, 2 * kk * planes, 0]) / cells
    return (new_field, energy)


def per_device(concentration):
    planes, rows, full_y = concentration.shape
    devices = lax.axis_size("slab") * lax.axis_size("section")
    share = full_y // 4 // devices
    fits = (
        rows == lanes
        and planes * lax.axis_size("section") == 4
        and 2 * share == row_group
        and devices % 8 == 0
        and lax.axis_size("slab") % 4 == 0
    )
    return kernel_step(concentration) if fits else plain_step(concentration)


def solution(mesh):
    return jax.shard_map(
        per_device,
        mesh=mesh,
        in_specs=(P("section", "slab", None),),
        out_specs=(P("section", "slab", None), P()),
        check_vma=False,
    )
```
